32 devices in a mesh: batch: 8 (over z, y), tok: 4 (over x, core).
Axes of the slice: x: 2, y: 2, z: 4, core: 2. Of those that a mesh axis runs over, the one named last changes fastest.
Arguments:
- tables: bfloat16 [48, 512, 128], P('tok'), may hold values from -3 to 3
- feature_ids: int32 [128, 48, 8], P('batch', 'tok'), may hold values from 0 to 511
- bag_lengths: int32 [128, 48], P('batch', 'tok'), may hold values from 1 to 8
- table_token: int32 [48], replicated, may hold values from 0 to 15, as said below
- projection: bfloat16 [16, 128, 1536], P('tok'), may hold values from -0.5 to 0.5
- mix_gain: float32 [16, 1536], P('tok'), may hold values from 0.5 to 1.5
- in_weight: bfloat16 [16, 1536, 6144], P('tok', None, 'batch'), may hold values from -0.15625 to 0.15625
- in_bias: float32 [16, 6144], P('tok', 'batch'), may hold values from -3 to 3
- out_weight: bfloat16 [16, 6144, 1536], P('tok', 'batch'), may hold values from -0.078125 to 0.078125
- out_bias: float32 [16, 1536], P('tok'), may hold values from -3 to 3
- out_gain: float32 [16, 1536], P('tok'), may hold values from 0.5 to 1.5
- upstream: bfloat16 [128, 16, 1536], P('batch', 'tok'), may hold values from -6 to 6
Outputs:
- result: bfloat16 [128, 16, 1536], P('batch', 'tok')
- grad_in: bfloat16 [16, 1536, 6144], P('tok', None, 'batch')
- grad_out: bfloat16 [16, 6144, 1536], P('tok', 'batch')
- grad_projection: float32 [16, 128, 1536], P('tok')
The draws below stay inside these ranges and needn't reach their ends.
Inputs may be any that keep to these rules, and one draw needn't show every extreme that they name: `table_token`: every token 0 to 15 is fed by at least one table.
All inputs are finite; a program needn't handle non-finite values.
Results may differ from the reference program's by a relative error of at most 0.02.
Values may be sent and summed in bfloat16 or wider, within the bound.
A program may use at most 128 MiB of HBM per device.

```python
import math
import jax
import jax.numpy as jnp
import numpy as np
from jax import lax

T_SIZE = 16
D = 1536
FF = 6144
E = 128
ROWS = 512
BAG = 8
B = 128
NF = 48


def draw_table_token(key, part):
    base_key = jax.random.fold_in(key, 31)
    key_one, key_two = jax.random.split(base_key)
    spread = jax.random.randint(key_one, (NF,), 0, T_SIZE)
    positions = jnp.arange(NF, dtype=jnp.int32)
    assigned = jnp.where(positions < T_SIZE, positions, spread)
    shuffle = jax.random.permutation(key_two, NF)
    return assigned[shuffle].astype(jnp.int32)


def with_ends(array, stream_key, smallest, top_value):
    shape = array.shape
    index_at = [jax.random.randint(jax.random.fold_in(stream_key, axis), (), 0, shape[axis]) for axis in range(len(shape))]
    array = array.at[tuple(index_at)].set(smallest)
    longest = shape.index(max(shape))
    index_at[longest] = (index_at[longest] + 1) % shape[longest]
    return array.at[tuple(index_at)].set(top_value)


def block_scale(rng, extent, cuts, least, high):
    def one(position, shards_of):
        steps = jax.random.uniform(jax.random.fold_in(jax.random.fold_in(rng, 6), position), (shards_of,), jnp.float32, least / len(cuts), high / len(cuts))
        return jnp.repeat(jnp.exp(steps), extent[position] // shards_of).reshape((-1,) + (1,) * (len(extent) - position - 1))

    factor_of = one(*cuts[0])
    for cut in cuts[1:]:
        factor_of = factor_of * one(*cut)
    return factor_of


def rank_table(count, skew):
    weights = [(1 << 20) // math.isqrt(standing ** skew) + 1 for standing in range(1, count + 1)]
    deviation = 1 + sum(weights) // (1 << 30)
    return np.cumsum(np.array([max(1, weight // deviation) for weight in weights]))


def ranked(key, extent, amount, slope):
    listing = rank_table(amount, slope)
    pick = jax.random.randint(jax.random.fold_in(key, 1), extent, 0, int(listing[amount - 1]))
    grade = jnp.searchsorted(jnp.asarray(listing, jnp.int32), pick, side="right")
    return jax.random.permutation(jax.random.fold_in(key, 2), amount)[grade].astype(jnp.int32)


def gaussian(rng, dims, scale, reach, cuts=(), kind=jnp.bfloat16):
    values = scale * jax.random.normal(rng, dims, jnp.float32)
    if cuts:
        values = values * block_scale(rng, dims, cuts, -0.22, 0.18)
    return jnp.clip(values, -reach, reach).astype(kind)


def setup_inputs(seed: int = 0) -> dict:
    key_list = jax.random.split(jax.random.key(seed), 13)
    tables = gaussian(key_list[0], (NF, ROWS, E), 0.5, 3.0, ((0, 4),))
    feature_ids = with_ends(ranked(key_list[1], (B, NF, BAG), ROWS, 2), jax.random.fold_in(key_list[1], 3), 0, ROWS - 1).astype(jnp.int32)
    bag_lengths = with_ends(jax.random.randint(key_list[2], (B, NF), 1, BAG + 1), jax.random.fold_in(key_list[2], 1), 1, BAG).astype(jnp.int32)
    table_token = draw_table_token(jax.random.fold_in(key_list[12], 71), 0)
    projection = gaussian(key_list[4], (T_SIZE, E, D), E ** -0.5, 0.5, ((0, 4),))
    mix_gain = jnp.clip(1.0 + 0.1 * jax.random.normal(key_list[5], (T_SIZE, D), jnp.float32), 0.5, 1.5)
    in_weight = gaussian(key_list[6], (T_SIZE, D, FF), D ** -0.5, 0.15625, ((0, 4), (2, 8)))
    in_bias = gaussian(key_list[7], (T_SIZE, FF), 0.5, 3.0, ((0, 4), (1, 8)), jnp.float32)
    out_weight = gaussian(key_list[8], (T_SIZE, FF, D), FF ** -0.5, 0.078125, ((0, 4), (1, 8)))
    out_bias = gaussian(key_list[9], (T_SIZE, D), 0.5, 3.0, ((0, 4),), jnp.float32)
    out_gain = jnp.clip(1.0 + 0.1 * jax.random.normal(key_list[10], (T_SIZE, D), jnp.float32), 0.5, 1.5)
    upstream = gaussian(key_list[11], (B, T_SIZE, D), 1.0, 6.0, ((0, 8), (1, 4)))
    return {"tables": tables, "feature_ids": feature_ids, "bag_lengths": bag_lengths, "table_token": table_token, "projection": projection, "mix_gain": mix_gain, "in_weight": in_weight, "in_bias": in_bias, "out_weight": out_weight, "out_bias": out_bias, "out_gain": out_gain, "upstream": upstream}


epsilon = 1e-05

def activate(values):
    return jax.nn.gelu(values, approximate=True)

def activate_slope(values):
    _, pullback = jax.vjp(activate, values)
    return pullback(jnp.ones_like(values))[0]

def normalize(values, gain):
    center = values - lax.optimization_barrier(jnp.mean(values, axis=-1, keepdims=True))
    scale_inv = lax.rsqrt(lax.optimization_barrier(jnp.mean(center * center, axis=-1, keepdims=True)) + epsilon)
    return center * scale_inv * gain

def normalize_back(values, gain, upper):
    center = values - lax.optimization_barrier(jnp.mean(values, axis=-1, keepdims=True))
    scale_inv = lax.rsqrt(lax.optimization_barrier(jnp.mean(center * center, axis=-1, keepdims=True)) + epsilon)
    unit = center * scale_inv
    scaled = upper * gain
    return scale_inv * (scaled - lax.optimization_barrier(jnp.mean(scaled, axis=-1, keepdims=True)) - unit * lax.optimization_barrier(jnp.mean(scaled * unit, axis=-1, keepdims=True)))

def pool_table(table_rows, row_index, bag_length):
    picked = jnp.take(table_rows, row_index, axis=0).astype(jnp.float32)
    keeper = (jnp.arange(row_index.shape[-1], dtype=jnp.int32)[None, :] < bag_length[:, None]).astype(jnp.float32)
    return lax.optimization_barrier(jnp.sum(picked * keeper[:, :, None], axis=1))

def per_token(element):
    normed_token, summed_token, mix_scale, first_weight, first_bias, second_weight, second_bias, out_scale, upper_token = element
    hidden_pre = jnp.dot(normed_token, first_weight, preferred_element_type=jnp.float32) + first_bias
    hidden = activate(hidden_pre).astype(jnp.bfloat16)
    output_pre = jnp.dot(hidden, second_weight, preferred_element_type=jnp.float32) + second_bias + normed_token.astype(jnp.float32)
    result_token = normalize(output_pre, out_scale).astype(jnp.bfloat16)
    upper_grad = normalize_back(output_pre, out_scale, upper_token.astype(jnp.float32)).astype(jnp.bfloat16)
    grad_second = jnp.dot(hidden.T, upper_grad, preferred_element_type=jnp.float32).astype(jnp.bfloat16)
    hidden_grad = (jnp.dot(upper_grad, second_weight.T, preferred_element_type=jnp.float32) * activate_slope(hidden_pre)).astype(jnp.bfloat16)
    grad_first = jnp.dot(normed_token.T, hidden_grad, preferred_element_type=jnp.float32).astype(jnp.bfloat16)
    normed_grad = jnp.dot(hidden_grad, first_weight.T, preferred_element_type=jnp.float32) + upper_grad.astype(jnp.float32)
    sum_grad = normalize_back(summed_token, mix_scale, normed_grad).astype(jnp.bfloat16)
    return (result_token, grad_first, grad_second, sum_grad)

def reference(tables, feature_ids, bag_lengths, table_token, projection, mix_gain, in_weight, in_bias, out_weight, out_bias, out_gain, upstream):
    pooled = lax.map(lambda element: pool_table(element[0], element[1], element[2]), (tables, jnp.transpose(feature_ids, (1, 0, 2)), jnp.transpose(bag_lengths)))
    selector = (table_token[:, None] == jnp.arange(T_SIZE, dtype=jnp.int32)[None, :]).astype(jnp.float32)
    grouped = jnp.einsum('fbc,ft->btc', pooled, selector, precision=lax.Precision.HIGHEST).astype(jnp.bfloat16)
    head_dim = D // T_SIZE
    tokens_in = jnp.einsum('btc,tcd->btd', grouped.astype(jnp.float32), projection.astype(jnp.float32), precision=lax.Precision.HIGHEST).astype(jnp.bfloat16)
    mixed = jnp.transpose(tokens_in.reshape(B, T_SIZE, T_SIZE, head_dim), (0, 2, 1, 3)).reshape(B, T_SIZE, D)
    summed = mixed.astype(jnp.float32) + tokens_in.astype(jnp.float32)
    normed = normalize(summed, mix_gain[None]).astype(jnp.bfloat16)
    result_t, grad_in, grad_out, sum_grad_t = lax.map(per_token, (jnp.transpose(normed, (1, 0, 2)), jnp.transpose(summed, (1, 0, 2)), mix_gain, in_weight, in_bias, out_weight, out_bias, out_gain, jnp.transpose(upstream, (1, 0, 2))))
    result = jnp.transpose(result_t, (1, 0, 2))
    sum_grad = jnp.transpose(sum_grad_t, (1, 0, 2))
    head_back = jnp.transpose(sum_grad.reshape(B, T_SIZE, T_SIZE, head_dim), (0, 2, 1, 3)).reshape(B, T_SIZE, D)
    token_grad = (sum_grad.astype(jnp.float32) + head_back.astype(jnp.float32)).astype(jnp.bfloat16)
    grad_projection = jnp.einsum('btc,btd->tcd', grouped.astype(jnp.float32), token_grad.astype(jnp.float32), precision=lax.Precision.HIGHEST)
    return (result, grad_in, grad_out, grad_projection)
```

```python
import functools
import math

import jax
import jax.numpy as jnp
from jax import lax
from jax.experimental import pallas as pl
from jax.experimental.pallas import tpu as pltpu
from jax.sharding import PartitionSpec as P

epsilon = 1e-05


def normalize(values, gain):
    center = values - jnp.mean(values, axis=-1, keepdims=True)
    scale_inv = lax.rsqrt(jnp.mean(center * center, axis=-1, keepdims=True) + epsilon)
    return center * scale_inv * gain


def normalize_back(values, gain, upper):
    center = values - jnp.mean(values, axis=-1, keepdims=True)
    scale_inv = lax.rsqrt(jnp.mean(center * center, axis=-1, keepdims=True) + epsilon)
    unit = center * scale_inv
    scaled = upper * gain
    return scale_inv * (
        scaled
        - jnp.mean(scaled, axis=-1, keepdims=True)
        - unit * jnp.mean(scaled * unit, axis=-1, keepdims=True)
    )


def pool_table(table_rows, row_index, bag_length):
    picked = jnp.take(table_rows, row_index, axis=0).astype(jnp.float32)
    keeper = (
        jnp.arange(row_index.shape[-1], dtype=jnp.int32)[None, :] < bag_length[:, None]
    ).astype(jnp.float32)
    return jnp.sum(picked * keeper[:, :, None], axis=1)


def remote(source, target, send, recv, peer):
    return pltpu.make_async_remote_copy(
        src_ref=source,
        dst_ref=target,
        send_sem=send,
        recv_sem=recv,
        device_id={"batch": peer},
        device_id_type=pl.DeviceIdType.MESH,
    )


class Ring:
    def __init__(self, count):
        self.far_count = count // 2
        rank = lax.axis_index("batch")
        self.far = rank // 2
        self.near = rank % 2
        self.partner = self.far * 2 + (1 - self.near)

    def after(self, step):
        return (self.far + step) % self.far_count

    def peer(self, step):
        return self.after(step) * 2 + self.near

    def greet(self):
        barrier = pltpu.get_barrier_semaphore()
        for device in [self.partner] + [self.peer(k) for k in range(1, self.far_count)]:
            pl.semaphore_signal(
                barrier, inc=1, device_id={"batch": device}, device_id_type=pl.DeviceIdType.MESH
            )
        pl.semaphore_wait(barrier, self.far_count)


class Gather:
    def __init__(self, ring, own, full, local_sem, far_send, far_recv, near_send, near_recv):
        self.ring, self.own, self.full = ring, own, full
        self.local_sem = local_sem
        self.far_send, self.far_recv = far_send, far_recv
        self.near_send, self.near_recv = near_send, near_recv

    def far_copy(self, t, k):
        ring = self.ring
        return remote(
            self.own.at[t],
            self.full.at[t, ring.near, ring.far],
            self.far_send.at[t, k - 1],
            self.far_recv.at[t, k - 1],
            ring.peer(k),
        )

    def own_copy(self, t):
        ring = self.ring
        return pltpu.make_async_copy(
            self.own.at[t], self.full.at[t, ring.near, ring.far], self.local_sem.at[t]
        )

    def near_copy(self, t):
        half = self.full.at[t, self.ring.near]
        return remote(half, half, self.near_send.at[t], self.near_recv.at[t], self.ring.partner)

    def start(self, t):
        for k in range(1, self.ring.far_count):
            self.far_copy(t, k).start()
        self.own_copy(t).start()

    def forward(self, t):
        ring = self.ring
        self.own_copy(t).wait()
        for k in range(1, ring.far_count):
            remote(
                self.own.at[t],
                self.full.at[t, ring.near, ring.after(ring.far_count - k)],
                self.far_send.at[t, k - 1],
                self.far_recv.at[t, k - 1],
                ring.peer(k),
            ).wait_recv()
        self.near_copy(t).start()

    def arrive(self, t):
        half = self.full.at[t, 1 - self.ring.near]
        remote(
            half, half, self.near_send.at[t], self.near_recv.at[t], self.ring.partner
        ).wait_recv()

    def finish(self, t):
        for k in range(1, self.ring.far_count):
            self.far_copy(t, k).wait_send()
        self.near_copy(t).wait_send()


class Scatter:
    def __init__(self, ring, part, first, pair, second, near_send, near_recv, far_send, far_recv):
        self.ring, self.part, self.first = ring, part, first
        self.pair, self.second = pair, second
        self.near_send, self.near_recv = near_send, near_recv
        self.far_send, self.far_recv = far_send, far_recv

    def near_copy(self, t):
        return remote(
            self.part.at[t, 1 - self.ring.near],
            self.first.at[t],
            self.near_send.at[t],
            self.near_recv.at[t],
            self.ring.partner,
        )

    def far_copy(self, t, k):
        return remote(
            self.pair.at[t, self.ring.after(k)],
            self.second.at[t, k - 1],
            self.far_send.at[t, k - 1],
            self.far_recv.at[t, k - 1],
            self.ring.peer(k),
        )

    def start(self, t):
        self.near_copy(t).start()

    def forward(self, t):
        self.near_copy(t).wait_recv()
        mine = self.part[t, self.ring.near].astype(jnp.float32)
        self.pair[t] = (mine + self.first[t].astype(jnp.float32)).astype(self.pair.dtype)
        for k in range(1, self.ring.far_count):
            self.far_copy(t, k).start()

    def total(self, t):
        ring = self.ring
        result = self.part[t, ring.near, ring.far].astype(jnp.float32)
        result = result + self.first[t, ring.far].astype(jnp.float32)
        for k in range(1, ring.far_count):
            self.far_copy(t, k).wait_recv()
            result = result + self.second[t, k - 1].astype(jnp.float32)
        return result

    def finish(self, t):
        self.near_copy(t).wait_send()
        for k in range(1, self.ring.far_count):
            self.far_copy(t, k).wait_send()


def tile_of(width):
    return 256 if width % 256 == 0 else 128


def block_kernel(
    count,
    normed_ref,
    summed_ref,
    mix_gain_ref,
    in_weight_ref,
    in_bias_ref,
    out_weight_ref,
    out_bias_ref,
    out_gain_ref,
    upstream_ref,
    result_ref,
    normed_all_ref,
    hidden_ref,
    upper_all_ref,
    hidden_grad_ref,
    sum_grad_ref,
    in_held,
    out_held,
    slope,
    upper_own,
    part_a,
    first_a,
    pair_a,
    second_a,
    part_b,
    first_b,
    pair_b,
    second_b,
    weight_sem,
    one_sem,
    many_sem,
):
    tokens, rows, width = normed_ref.shape
    units = in_held.shape[-1]
    examples = count * rows
    far_count = count // 2
    ring = Ring(count)
    in_copy = lambda t: pltpu.make_async_copy(in_weight_ref.at[t], in_held.at[t], weight_sem.at[0, t])
    out_copy = lambda t: pltpu.make_async_copy(
        out_weight_ref.at[t], out_held.at[t], weight_sem.at[1, t]
    )
    for t in range(tokens):
        in_copy(t).start()
        out_copy(t).start()
    one = [one_sem.at[i] for i in range(10)]
    many = [many_sem.at[i] for i in range(8)]
    gather_a = Gather(
        ring, normed_ref, normed_all_ref, one[0], many[0], many[1], one[1], one[2]
    )
    gather_b = Gather(
        ring, upper_own, upper_all_ref, one[3], many[2], many[3], one[4], one[5]
    )
    scatter_a = Scatter(
        ring, part_a, first_a, pair_a, second_a, one[6], one[7], many[4], many[5]
    )
    scatter_b = Scatter(
        ring, part_b, first_b, pair_b, second_b, one[8], one[9], many[6], many[7]
    )
    ring.greet()
    for t in range(tokens):
        gather_a.start(t)

    unit_tile = tile_of(units)
    width_tile = tile_of(width)

    def forward(t):
        in_copy(t).wait()
        out_copy(t).wait()
        gather_a.arrive(t)

        @pl.loop(0, units // unit_tile)
        def _(i):
            columns = pl.ds(pl.multiple_of(i * unit_tile, unit_tile), unit_tile)
            value = jnp.dot(
                normed_all_ref[t].reshape(examples, width),
                in_held[t, :, columns],
                preferred_element_type=jnp.float32,
            ) + in_bias_ref[t, :, columns]
            factor = math.sqrt(2 / math.pi)
            square = value * value
            bent = jnp.tanh(factor * (value + 0.044715 * value * square))
            hidden_ref[t, :, columns] = (0.5 * value * (1 + bent)).astype(jnp.bfloat16)
            slope[t, :, columns] = 0.5 * (1 + bent) + 0.5 * value * (1 - bent * bent) * factor * (
                1 + 3 * 0.044715 * square
            )

        @pl.loop(0, width // width_tile)
        def _(i):
            columns = pl.ds(pl.multiple_of(i * width_tile, width_tile), width_tile)
            value = jnp.dot(
                hidden_ref[t], out_held[t, :, columns], preferred_element_type=jnp.float32
            )
            part_a[t, :, :, :, columns] = value.astype(jnp.bfloat16).reshape(
                2, far_count, rows, width_tile
            )

        scatter_a.start(t)

    def turn(t):
        output = scatter_a.total(t) + out_bias_ref[t] + normed_ref[t].astype(jnp.float32)
        center = output - jnp.mean(output, axis=-1, keepdims=True)
        scale_inv = lax.rsqrt(jnp.mean(center * center, axis=-1, keepdims=True) + epsilon)
        result_ref[t] = (center * scale_inv * out_gain_ref[t]).astype(jnp.bfloat16)
        upper_own[t] = normalize_back(
            output, out_gain_ref[t], upstream_ref[t].astype(jnp.float32)
        ).astype(jnp.bfloat16)
        gather_b.start(t)

    def backward(t):
        gather_b.arrive(t)

        @pl.loop(0, units // unit_tile)
        def _(i):
            columns = pl.ds(pl.multiple_of(i * unit_tile, unit_tile), unit_tile)
            value = lax.dot_general(
                upper_all_ref[t].reshape(examples, width),
                out_held[t, columns, :],
                (((1,), (1,)), ((), ())),
                preferred_element_type=jnp.float32,
            )
            hidden_grad_ref[t, :, columns] = (value * slope[t, :, columns]).astype(jnp.bfloat16)

        @pl.loop(0, width // width_tile)
        def _(i):
            columns = pl.ds(pl.multiple_of(i * width_tile, width_tile), width_tile)
            value = lax.dot_general(
                hidden_grad_ref[t],
                in_held[t, columns, :],
                (((1,), (1,)), ((), ())),
                preferred_element_type=jnp.float32,
            )
            part_b[t, :, :, :, columns] = value.astype(jnp.bfloat16).reshape(
                2, far_count, rows, width_tile
            )

        scatter_b.start(t)

    def close(t):
        normed_grad = scatter_b.total(t) + upper_own[t].astype(jnp.float32)
        sum_grad_ref[t] = normalize_back(summed_ref[t], mix_gain_ref[t], normed_grad).astype(
            jnp.bfloat16
        )

    stages = [
        gather_a.forward,
        forward,
        scatter_a.forward,
        turn,
        gather_b.forward,
        backward,
        scatter_b.forward,
        close,
    ]

    def step(s, carry):
        for delay, stage in enumerate(stages):

            @pl.when(jnp.logical_and(s >= delay, s < delay + tokens))
            def _():
                stage(s - delay)

        return carry

    lax.fori_loop(0, tokens + len(stages) - 1, step, 0)
    for t in range(tokens):
        for part in (gather_a, scatter_a, gather_b, scatter_b):
            part.finish(t)


def run_block(count, *operands):
    tokens, rows, width = operands[0].shape
    units = operands[3].shape[-1]
    far_count = count // 2
    half = jnp.bfloat16
    vmem = pl.BlockSpec(memory_space=pltpu.VMEM)
    anywhere = pl.BlockSpec(memory_space=pl.ANY)
    full = (tokens, 2, far_count, rows, width)
    one_way = [
        pltpu.VMEM(full, half),
        pltpu.VMEM((tokens, far_count, rows, width), half),
        pltpu.VMEM((tokens, far_count, rows, width), half),
        pltpu.VMEM((tokens, far_count - 1, rows, width), half),
    ]
    examples = count * rows
    return pl.pallas_call(
        functools.partial(block_kernel, count),
        out_shape=[
            jax.ShapeDtypeStruct((tokens, rows, width), half),
            jax.ShapeDtypeStruct(full, half),
            jax.ShapeDtypeStruct((tokens, examples, units), half),
            jax.ShapeDtypeStruct(full, half),
            jax.ShapeDtypeStruct((tokens, examples, units), half),
            jax.ShapeDtypeStruct((tokens, rows, width), half),
        ],
        in_specs=[vmem, vmem, vmem, anywhere, vmem, anywhere, vmem, vmem, vmem],
        out_specs=[vmem] * 6,
        scratch_shapes=[
            pltpu.VMEM((tokens, width, units), half),
            pltpu.VMEM((tokens, units, width), half),
            pltpu.VMEM((tokens, examples, units), jnp.float32),
            pltpu.VMEM((tokens, rows, width), half),
            *one_way,
            *one_way,
            pltpu.SemaphoreType.DMA((2, tokens)),
            pltpu.SemaphoreType.DMA((10, tokens)),
            pltpu.SemaphoreType.DMA((8, tokens, far_count - 1)),
        ],
        compiler_params=pltpu.CompilerParams(
            collective_id=0, has_side_effects=True, vmem_limit_bytes=50 * 1024 * 1024
        ),
        name="block",
    )(*operands)


def gather_kernel(count, own_ref, full_ref, one_sem, many_sem):
    ring = Ring(count)
    gather = Gather(
        ring, own_ref, full_ref, one_sem.at[0], many_sem.at[0], many_sem.at[1], one_sem.at[1],
        one_sem.at[2],
    )
    ring.greet()
    tokens = own_ref.shape[0]
    for t in range(tokens):
        gather.start(t)
    for t in range(tokens):
        gather.forward(t)
    for t in range(tokens):
        gather.arrive(t)
        gather.finish(t)


def run_gather(count, own):
    tokens, rows, width = own.shape
    far_count = count // 2
    vmem = pl.BlockSpec(memory_space=pltpu.VMEM)
    return pl.pallas_call(
        functools.partial(gather_kernel, count),
        out_shape=jax.ShapeDtypeStruct((tokens, 2, far_count, rows, width), own.dtype),
        in_specs=[vmem],
        out_specs=vmem,
        scratch_shapes=[
            pltpu.SemaphoreType.DMA((3, tokens)),
            pltpu.SemaphoreType.DMA((2, tokens, far_count - 1)),
        ],
        compiler_params=pltpu.CompilerParams(
            collective_id=1, has_side_effects=True, vmem_limit_bytes=16 * 1024 * 1024
        ),
        name="gather",
    )(own)


def local(
    tables,
    feature_ids,
    bag_lengths,
    table_token,
    projection,
    mix_gain,
    in_weight,
    in_bias,
    out_weight,
    out_bias,
    out_gain,
    upstream,
):
    token_rank = lax.axis_index("tok")
    count = lax.axis_size("batch")
    local_tokens, embed_width, model_width = projection.shape
    all_tokens = local_tokens * lax.axis_size("tok")
    head_dim = model_width // all_tokens
    local_tables, table_rows, _ = tables.shape
    local_rows = feature_ids.shape[0]
    keeper = jnp.arange(feature_ids.shape[-1], dtype=jnp.int32) < bag_lengths[:, :, None]
    chosen = jnp.where(keeper, feature_ids, -1)
    uses = jnp.sum(
        (chosen[:, :, :, None] == jnp.arange(table_rows, dtype=jnp.int32)).astype(jnp.float32),
        axis=2,
    ).astype(jnp.bfloat16)
    pooled = jnp.einsum("bfr,frc->fbc", uses, tables, preferred_element_type=jnp.float32)
    local_owner = lax.dynamic_slice_in_dim(table_token, token_rank * local_tables, local_tables)
    selector = (local_owner[:, None] == jnp.arange(all_tokens, dtype=jnp.int32)[None, :]).astype(
        jnp.float32
    )
    partial_groups = jnp.einsum("fbc,ft->tbc", pooled, selector, precision=lax.Precision.HIGHEST)
    group_all = lax.psum(partial_groups, "tok").astype(jnp.bfloat16)
    grouped = lax.dynamic_slice_in_dim(group_all, token_rank * local_tokens, local_tokens, 0)
    own_tokens = jnp.einsum(
        "tbc,tcd->tbd", grouped, projection, preferred_element_type=jnp.float32
    ).astype(jnp.bfloat16)

    def exchange(values):
        blocks = values.reshape(local_tokens, local_rows, all_tokens, head_dim)
        moved = lax.all_to_all(blocks, "tok", split_axis=2, concat_axis=0, tiled=True)
        return jnp.transpose(moved, (2, 1, 0, 3)).reshape(values.shape)

    summed = exchange(own_tokens).astype(jnp.float32) + own_tokens.astype(jnp.float32)
    normed = normalize(summed, mix_gain[:, None]).astype(jnp.bfloat16)
    result, normed_all, hidden, upper_all, hidden_grad, sum_grad = run_block(
        count,
        normed,
        summed,
        mix_gain[:, None],
        in_weight,
        in_bias[:, None],
        out_weight,
        out_bias[:, None],
        out_gain[:, None],
        jnp.transpose(upstream, (1, 0, 2)),
    )
    flat = (local_tokens, count * local_rows, model_width)
    grad_out = jnp.einsum(
        "tbf,tbd->tfd", hidden, upper_all.reshape(flat), preferred_element_type=jnp.float32
    ).astype(jnp.bfloat16)
    grad_in = jnp.einsum(
        "tbd,tbf->tdf", normed_all.reshape(flat), hidden_grad, preferred_element_type=jnp.float32
    ).astype(jnp.bfloat16)
    token_grad = (
        sum_grad.astype(jnp.float32) + exchange(sum_grad).astype(jnp.float32)
    ).astype(jnp.bfloat16)
    both = run_gather(count, jnp.concatenate([token_grad, grouped], axis=-1))
    both = both.reshape(local_tokens, count * local_rows, model_width + embed_width)
    grad_projection = jnp.einsum(
        "tbc,tbd->tcd",
        both[..., model_width:],
        both[..., :model_width],
        preferred_element_type=jnp.float32,
    )
    return (jnp.transpose(result, (1, 0, 2)), grad_in, grad_out, grad_projection)


def solution(mesh):
    in_specs = (
        P("tok", None, None),
        P("batch", "tok", None),
        P("batch", "tok"),
        P(),
        P("tok", None, None),
        P("tok", None),
        P("tok", None, "batch"),
        P("tok", "batch"),
        P("tok", "batch", None),
        P("tok", None),
        P("tok", None),
        P("batch", "tok", None),
    )
    out_specs = (
        P("batch", "tok", None),
        P("tok", None, "batch"),
        P("tok", "batch", None),
        P("tok", None, None),
    )
    return jax.shard_map(local, mesh=mesh, in_specs=in_specs, out_specs=out_specs, check_vma=False)
```

```python
import functools
import math

import jax
import jax.numpy as jnp
from jax import lax
from jax.experimental import pallas as pl
from jax.experimental.pallas import tpu as pltpu
from jax.sharding import PartitionSpec as P

epsilon = 1e-05


def normalize(values, gain):
    center = values - jnp.mean(values, axis=-1, keepdims=True)
    scale_inv = lax.rsqrt(jnp.mean(center * center, axis=-1, keepdims=True) + epsilon)
    return center * scale_inv * gain


def normalize_back(values, gain, upper):
    center = values - jnp.mean(values, axis=-1, keepdims=True)
    scale_inv = lax.rsqrt(jnp.mean(center * center, axis=-1, keepdims=True) + epsilon)
    unit = center * scale_inv
    scaled = upper * gain
    return scale_inv * (
        scaled
        - jnp.mean(scaled, axis=-1, keepdims=True)
        - unit * jnp.mean(scaled * unit, axis=-1, keepdims=True)
    )


def pool_table(table_rows, row_index, bag_length):
    picked = jnp.take(table_rows, row_index, axis=0).astype(jnp.float32)
    keeper = (
        jnp.arange(row_index.shape[-1], dtype=jnp.int32)[None, :] < bag_length[:, None]
    ).astype(jnp.float32)
    return jnp.sum(picked * keeper[:, :, None], axis=1)


def remote(source, target, send, recv, peer, axis="batch"):
    return pltpu.make_async_remote_copy(
        src_ref=source,
        dst_ref=target,
        send_sem=send,
        recv_sem=recv,
        device_id={axis: peer},
        device_id_type=pl.DeviceIdType.MESH,
    )


class Ring:
    def __init__(self, count):
        self.far_count = count // 2
        rank = lax.axis_index("batch")
        self.far = rank // 2
        self.near = rank % 2
        self.partner = self.far * 2 + (1 - self.near)

    def after(self, step):
        return (self.far + step) % self.far_count

    def peer(self, step):
        return self.after(step) * 2 + self.near

    def greet(self):
        barrier = pltpu.get_barrier_semaphore()
        for device in [self.partner] + [self.peer(k) for k in range(1, self.far_count)]:
            pl.semaphore_signal(
                barrier, inc=1, device_id={"batch": device}, device_id_type=pl.DeviceIdType.MESH
            )
        pl.semaphore_wait(barrier, self.far_count)


class Gather:
    def __init__(self, ring, own, full, one, many):
        self.ring, self.own, self.full = ring, own, full
        self.local_sem, self.pass_send, self.pass_recv = one
        self.far_send, self.far_recv, self.near_send, self.near_recv = many

    def far_copy(self, t, k):
        ring = self.ring
        return remote(
            self.own.at[t],
            self.full.at[t, ring.near, ring.far],
            self.far_send.at[t, k - 1],
            self.far_recv.at[t, k - 1],
            ring.peer(k),
        )

    def pass_copy(self, t, near):
        ring = self.ring
        return remote(
            self.own.at[t],
            self.full.at[t, near, ring.far],
            self.pass_send.at[t],
            self.pass_recv.at[t],
            ring.partner,
        )

    def own_copy(self, t):
        ring = self.ring
        return pltpu.make_async_copy(
            self.own.at[t], self.full.at[t, ring.near, ring.far], self.local_sem.at[t]
        )

    def near_copy(self, t, k, near):
        ring = self.ring
        block = self.full.at[t, near, ring.after(ring.far_count - k)]
        return remote(
            block, block, self.near_send.at[t, k - 1], self.near_recv.at[t, k - 1], ring.partner
        )

    def start(self, t):
        for k in range(1, self.ring.far_count):
            self.far_copy(t, k).start()
        self.pass_copy(t, self.ring.near).start()
        self.own_copy(t).start()

    def forward(self, t):
        ring = self.ring
        for k in range(1, ring.far_count):
            remote(
                self.own.at[t],
                self.full.at[t, ring.near, ring.after(ring.far_count - k)],
                self.far_send.at[t, k - 1],
                self.far_recv.at[t, k - 1],
                ring.peer(k),
            ).wait_recv()
            self.near_copy(t, k, ring.near).start()

    def arrive(self, t):
        self.own_copy(t).wait()
        self.pass_copy(t, 1 - self.ring.near).wait_recv()
        for k in range(1, self.ring.far_count):
            self.near_copy(t, k, 1 - self.ring.near).wait_recv()

    def finish(self, t):
        self.pass_copy(t, self.ring.near).wait_send()
        for k in range(1, self.ring.far_count):
            self.far_copy(t, k).wait_send()
            self.near_copy(t, k, self.ring.near).wait_send()


class Scatter:
    def __init__(self, ring, part, first, pair, second, near_send, near_recv, far_send, far_recv):
        self.ring, self.part, self.first = ring, part, first
        self.pair, self.second = pair, second
        self.near_send, self.near_recv = near_send, near_recv
        self.far_send, self.far_recv = far_send, far_recv

    def near_copy(self, t):
        return remote(
            self.part.at[t, 1 - self.ring.near],
            self.first.at[t],
            self.near_send.at[t],
            self.near_recv.at[t],
            self.ring.partner,
        )

    def far_copy(self, t, k):
        return remote(
            self.pair.at[t, self.ring.after(k)],
            self.second.at[t, k - 1],
            self.far_send.at[t, k - 1],
            self.far_recv.at[t, k - 1],
            self.ring.peer(k),
        )

    def start(self, t):
        self.near_copy(t).start()

    def forward(self, t):
        self.near_copy(t).wait_recv()
        mine = self.part[t, self.ring.near].astype(jnp.float32)
        self.pair[t] = (mine + self.first[t].astype(jnp.float32)).astype(self.pair.dtype)
        for k in range(1, self.ring.far_count):
            self.far_copy(t, k).start()

    def total(self, t):
        ring = self.ring
        result = self.part[t, ring.near, ring.far].astype(jnp.float32)
        result = result + self.first[t, ring.far].astype(jnp.float32)
        for k in range(1, ring.far_count):
            self.far_copy(t, k).wait_recv()
            result = result + self.second[t, k - 1].astype(jnp.float32)
        return result

    def finish(self, t):
        self.near_copy(t).wait_send()
        for k in range(1, self.ring.far_count):
            self.far_copy(t, k).wait_send()


def tile_of(width):
    return 256 if width % 256 == 0 else 128


def block_kernel(
    count,
    normed_ref,
    summed_ref,
    mix_gain_ref,
    in_weight_ref,
    in_bias_ref,
    out_weight_ref,
    out_bias_ref,
    out_gain_ref,
    upstream_ref,
    result_ref,
    normed_all_ref,
    hidden_ref,
    upper_all_ref,
    hidden_grad_ref,
    sum_grad_ref,
    in_held,
    out_held,
    slope,
    upper_own,
    part_a,
    first_a,
    pair_a,
    second_a,
    part_b,
    first_b,
    pair_b,
    second_b,
    weight_sem,
    one_sem,
    many_sem,
):
    tokens, rows, width = normed_ref.shape
    units = in_held.shape[-1]
    examples = count * rows
    far_count = count // 2
    ring = Ring(count)
    in_copy = lambda t: pltpu.make_async_copy(in_weight_ref.at[t], in_held.at[t], weight_sem.at[0, t])
    out_copy = lambda t: pltpu.make_async_copy(
        out_weight_ref.at[t], out_held.at[t], weight_sem.at[1, t]
    )
    for t in range(tokens):
        in_copy(t).start()
        out_copy(t).start()
    one = [one_sem.at[i] for i in range(10)]
    many = [many_sem.at[i] for i in range(12)]
    gather_a = Gather(ring, normed_ref, normed_all_ref, one[0:3], many[0:4])
    gather_b = Gather(ring, upper_own, upper_all_ref, one[3:6], many[8:12])
    scatter_a = Scatter(
        ring, part_a, first_a, pair_a, second_a, one[6], one[7], many[4], many[5]
    )
    scatter_b = Scatter(
        ring, part_b, first_b, pair_b, second_b, one[8], one[9], many[6], many[7]
    )
    ring.greet()
    for t in range(tokens):
        gather_a.start(t)

    unit_tile = tile_of(units)
    width_tile = tile_of(width)

    def forward(t):
        in_copy(t).wait()
        out_copy(t).wait()
        gather_a.arrive(t)

        @pl.loop(0, units // unit_tile)
        def _(i):
            columns = pl.ds(pl.multiple_of(i * unit_tile, unit_tile), unit_tile)
            value = jnp.dot(
                normed_all_ref[t].reshape(examples, width),
                in_held[t, :, columns],
                preferred_element_type=jnp.float32,
            ) + in_bias_ref[pl.ds(t, 1), columns]
            factor = math.sqrt(2 / math.pi)
            square = value * value
            bent = jnp.tanh(factor * (value + 0.044715 * value * square))
            hidden_ref[t, :, columns] = (0.5 * value * (1 + bent)).astype(jnp.bfloat16)
            slope[t, :, columns] = 0.5 * (1 + bent) + 0.5 * value * (1 - bent * bent) * factor * (
                1 + 3 * 0.044715 * square
            )

        @pl.loop(0, width // width_tile)
        def _(i):
            columns = pl.ds(pl.multiple_of(i * width_tile, width_tile), width_tile)
            value = jnp.dot(
                hidden_ref[t], out_held[t, :, columns], preferred_element_type=jnp.float32
            )
            part_a[t, :, :, :, columns] = value.astype(jnp.bfloat16).reshape(
                2, far_count, rows, width_tile
            )

        scatter_a.start(t)

    def turn(t):
        output = scatter_a.total(t) + out_bias_ref[pl.ds(t, 1), :] + normed_ref[t].astype(jnp.float32)
        center = output - jnp.mean(output, axis=-1, keepdims=True)
        scale_inv = lax.rsqrt(jnp.mean(center * center, axis=-1, keepdims=True) + epsilon)
        result_ref[t] = (center * scale_inv * out_gain_ref[pl.ds(t, 1), :]).astype(jnp.bfloat16)
        upper_own[t] = normalize_back(
            output, out_gain_ref[pl.ds(t, 1), :], upstream_ref[t].astype(jnp.float32)
        ).astype(jnp.bfloat16)
        gather_b.start(t)

    def backward(t):
        gather_b.arrive(t)

        @pl.loop(0, units // unit_tile)
        def _(i):
            columns = pl.ds(pl.multiple_of(i * unit_tile, unit_tile), unit_tile)
            value = lax.dot_general(
                upper_all_ref[t].reshape(examples, width),
                out_held[t, columns, :],
                (((1,), (1,)), ((), ())),
                preferred_element_type=jnp.float32,
            )
            hidden_grad_ref[t, :, columns] = (value * slope[t, :, columns]).astype(jnp.bfloat16)

        @pl.loop(0, width // width_tile)
        def _(i):
            columns = pl.ds(pl.multiple_of(i * width_tile, width_tile), width_tile)
            value = lax.dot_general(
                hidden_grad_ref[t],
                in_held[t, columns, :],
                (((1,), (1,)), ((), ())),
                preferred_element_type=jnp.float32,
            )
            part_b[t, :, :, :, columns] = value.astype(jnp.bfloat16).reshape(
                2, far_count, rows, width_tile
            )

        scatter_b.start(t)

    def close(t):
        normed_grad = scatter_b.total(t) + upper_own[t].astype(jnp.float32)
        sum_grad_ref[t] = normalize_back(summed_ref[t], mix_gain_ref[pl.ds(t, 1), :], normed_grad).astype(
            jnp.bfloat16
        )

    stages = [
        gather_a.forward,
        forward,
        scatter_a.forward,
        turn,
        gather_b.forward,
        backward,
        scatter_b.forward,
        close,
    ]

    def step(s, carry):
        for delay, stage in enumerate(stages):

            @pl.when(jnp.logical_and(s >= delay, s < delay + tokens))
            def _():
                stage(s - delay)

        return carry

    lax.fori_loop(0, tokens + len(stages) - 1, step, 0)
    for t in range(tokens):
        for part in (gather_a, scatter_a, gather_b, scatter_b):
            part.finish(t)


def run_block(count, *operands):
    tokens, rows, width = operands[0].shape
    units = operands[3].shape[-1]
    far_count = count // 2
    half = jnp.bfloat16
    vmem = pl.BlockSpec(memory_space=pltpu.VMEM)
    anywhere = pl.BlockSpec(memory_space=pl.ANY)
    full = (tokens, 2, far_count, rows, width)
    one_way = [
        pltpu.VMEM(full, half),
        pltpu.VMEM((tokens, far_count, rows, width), half),
        pltpu.VMEM((tokens, far_count, rows, width), half),
        pltpu.VMEM((tokens, far_count - 1, rows, width), half),
    ]
    examples = count * rows
    return pl.pallas_call(
        functools.partial(block_kernel, count),
        out_shape=[
            jax.ShapeDtypeStruct((tokens, rows, width), half),
            jax.ShapeDtypeStruct(full, half),
            jax.ShapeDtypeStruct((tokens, examples, units), half),
            jax.ShapeDtypeStruct(full, half),
            jax.ShapeDtypeStruct((tokens, examples, units), half),
            jax.ShapeDtypeStruct((tokens, rows, width), half),
        ],
        in_specs=[vmem, vmem, vmem, anywhere, vmem, anywhere, vmem, vmem, vmem],
        out_specs=[vmem] * 6,
        scratch_shapes=[
            pltpu.VMEM((tokens, width, units), half),
            pltpu.VMEM((tokens, units, width), half),
            pltpu.VMEM((tokens, examples, units), jnp.float32),
            pltpu.VMEM((tokens, rows, width), half),
            *one_way,
            *one_way,
            pltpu.SemaphoreType.DMA((2, tokens)),
            pltpu.SemaphoreType.DMA((10, tokens)),
            pltpu.SemaphoreType.DMA((12, tokens, far_count - 1)),
        ],
        compiler_params=pltpu.CompilerParams(
            collective_id=0, has_side_effects=True, vmem_limit_bytes=50 * 1024 * 1024
        ),
        name="block",
    )(*operands)


def gather_kernel(count, own_ref, full_ref, one_sem, many_sem):
    ring = Ring(count)
    gather = Gather(
        ring,
        own_ref,
        full_ref,
        [one_sem.at[i] for i in range(3)],
        [many_sem.at[i] for i in range(4)],
    )
    ring.greet()
    tokens = own_ref.shape[0]
    for t in range(tokens):
        gather.start(t)
    for t in range(tokens):
        gather.forward(t)
    for t in range(tokens):
        gather.arrive(t)
        gather.finish(t)


def run_gather(count, own):
    tokens, rows, width = own.shape
    far_count = count // 2
    vmem = pl.BlockSpec(memory_space=pltpu.VMEM)
    return pl.pallas_call(
        functools.partial(gather_kernel, count),
        out_shape=jax.ShapeDtypeStruct((tokens, 2, far_count, rows, width), own.dtype),
        in_specs=[vmem],
        out_specs=vmem,
        scratch_shapes=[
            pltpu.SemaphoreType.DMA((3, tokens)),
            pltpu.SemaphoreType.DMA((4, tokens, far_count - 1)),
        ],
        compiler_params=pltpu.CompilerParams(
            collective_id=1, has_side_effects=True, vmem_limit_bytes=16 * 1024 * 1024
        ),
        name="gather",
    )(own)


def mix_kernel(
    peers,
    part_ref,
    projection_ref,
    grouped_ref,
    own_ref,
    moved_ref,
    arrived,
    blocks,
    sems,
):
    rank = lax.axis_index("tok")
    tokens, _, width = projection_ref.shape
    piece = width // peers
    after = lambda step: (rank + step) % peers
    barrier = pltpu.get_barrier_semaphore()
    for k in range(1, peers):
        pl.semaphore_signal(
            barrier, inc=1, device_id={"tok": after(k)}, device_id_type=pl.DeviceIdType.MESH
        )
    pl.semaphore_wait(barrier, peers - 1)

    def part_copy(k):
        return remote(
            part_ref.at[after(k)],
            arrived.at[k - 1],
            sems.at[0, k - 1],
            sems.at[1, k - 1],
            after(k),
            "tok",
        )

    def slice_copy(k, slot):
        return remote(
            blocks.at[after(k)],
            moved_ref.at[slot],
            sems.at[2, k - 1],
            sems.at[3, k - 1],
            after(k),
            "tok",
        )

    for k in range(1, peers):
        part_copy(k).start()
    total = part_ref[rank]
    for k in range(1, peers):
        part_copy(k).wait_recv()
        total = total + arrived[k - 1]
    grouped_ref[...] = total.astype(jnp.bfloat16)
    for t in range(tokens):
        value = jnp.dot(
            grouped_ref[t], projection_ref[t], preferred_element_type=jnp.float32
        ).astype(jnp.bfloat16)
        own_ref[t] = value
        for peer in range(peers):
            blocks[peer, t] = value[:, peer * piece : (peer + 1) * piece]
    for k in range(1, peers):
        slice_copy(k, rank).start()
    moved_ref[rank] = blocks[rank]
    for k in range(1, peers):
        slice_copy(k, after(peers - k)).wait_recv()
    for k in range(1, peers):
        part_copy(k).wait_send()
        slice_copy(k, rank).wait_send()


def run_mix(peers, part, projection):
    tokens, embed, width = projection.shape
    rows = part.shape[1]
    vmem = pl.BlockSpec(memory_space=pltpu.VMEM)
    moved = (peers, tokens, rows, width // peers)
    return pl.pallas_call(
        functools.partial(mix_kernel, peers),
        out_shape=[
            jax.ShapeDtypeStruct((tokens, rows, embed), jnp.bfloat16),
            jax.ShapeDtypeStruct((tokens, rows, width), jnp.bfloat16),
            jax.ShapeDtypeStruct(moved, jnp.bfloat16),
        ],
        in_specs=[vmem] * 2,
        out_specs=[vmem] * 3,
        scratch_shapes=[
            pltpu.VMEM((peers - 1, tokens, rows, embed), jnp.float32),
            pltpu.VMEM(moved, jnp.bfloat16),
            pltpu.SemaphoreType.DMA((4, peers - 1)),
        ],
        compiler_params=pltpu.CompilerParams(
            collective_id=2, has_side_effects=True, vmem_limit_bytes=16 * 1024 * 1024
        ),
        name="mix",
    )(part.reshape(peers, tokens, rows, embed), projection)


def local(
    tables,
    feature_ids,
    bag_lengths,
    table_token,
    projection,
    mix_gain,
    in_weight,
    in_bias,
    out_weight,
    out_bias,
    out_gain,
    upstream,
):
    token_rank = lax.axis_index("tok")
    count = lax.axis_size("batch")
    local_tokens, embed_width, model_width = projection.shape
    all_tokens = local_tokens * lax.axis_size("tok")
    head_dim = model_width // all_tokens
    local_tables, table_rows, _ = tables.shape
    local_rows = feature_ids.shape[0]
    keeper = jnp.arange(feature_ids.shape[-1], dtype=jnp.int32) < bag_lengths[:, :, None]
    chosen = jnp.where(keeper, feature_ids, -1)
    uses = jnp.sum(
        (chosen[:, :, :, None] == jnp.arange(table_rows, dtype=jnp.int32)).astype(jnp.float32),
        axis=2,
    ).astype(jnp.bfloat16)
    pooled = jnp.einsum("bfr,frc->fbc", uses, tables, preferred_element_type=jnp.float32)
    local_owner = lax.dynamic_slice_in_dim(table_token, token_rank * local_tables, local_tables)
    selector = (local_owner[:, None] == jnp.arange(all_tokens, dtype=jnp.int32)[None, :]).astype(
        jnp.float32
    )
    partial_groups = jnp.einsum("fbc,ft->tbc", pooled, selector, precision=lax.Precision.HIGHEST)
    grouped, own_tokens, moved_tokens = run_mix(lax.axis_size("tok"), partial_groups, projection)

    def unfold(moved):
        blocks = moved.reshape(all_tokens, local_rows, local_tokens, head_dim)
        return jnp.transpose(blocks, (2, 1, 0, 3)).reshape(local_tokens, local_rows, model_width)

    def exchange(values):
        blocks = values.reshape(local_tokens, local_rows, all_tokens, head_dim)
        moved = lax.all_to_all(blocks, "tok", split_axis=2, concat_axis=0, tiled=True)
        return unfold(moved)

    summed = unfold(moved_tokens).astype(jnp.float32) + own_tokens.astype(jnp.float32)
    normed = normalize(summed, mix_gain[:, None]).astype(jnp.bfloat16)
    result, normed_all, hidden, upper_all, hidden_grad, sum_grad = run_block(
        count,
        normed,
        summed,
        mix_gain,
        in_weight,
        in_bias,
        out_weight,
        out_bias,
        out_gain,
        jnp.transpose(upstream, (1, 0, 2)),
    )
    flat = (local_tokens, count * local_rows, model_width)
    grad_out = jnp.einsum(
        "tbf,tbd->tfd", hidden, upper_all.reshape(flat), preferred_element_type=jnp.float32
    ).astype(jnp.bfloat16)
    grad_in = jnp.einsum(
        "tbd,tbf->tdf", normed_all.reshape(flat), hidden_grad, preferred_element_type=jnp.float32
    ).astype(jnp.bfloat16)
    token_grad = (
        sum_grad.astype(jnp.float32) + exchange(sum_grad).astype(jnp.float32)
    ).astype(jnp.bfloat16)
    both = run_gather(count, jnp.concatenate([token_grad, grouped], axis=-1))
    both = both.reshape(local_tokens, count * local_rows, model_width + embed_width)
    grad_projection = jnp.einsum(
        "tbc,tbd->tcd",
        both[..., model_width:],
        both[..., :model_width],
        preferred_element_type=jnp.float32,
    )
    return (jnp.transpose(result, (1, 0, 2)), grad_in, grad_out, grad_projection)


def solution(mesh):
    in_specs = (
        P("tok", None, None),
        P("batch", "tok", None),
        P("batch", "tok"),
        P(),
        P("tok", None, None),
        P("tok", None),
        P("tok", None, "batch"),
        P("tok", "batch"),
        P("tok", "batch", None),
        P("tok", None),
        P("tok", None),
        P("batch", "tok", None),
    )
    out_specs = (
        P("batch", "tok", None),
        P("tok", None, "batch"),
        P("tok", "batch", None),
        P("tok", None, None),
    )
    return jax.shard_map(local, mesh=mesh, in_specs=in_specs, out_specs=out_specs, check_vma=False)
```
